32 devices in a mesh: gx: 4 (over z), gy: 2 (over x), gz: 4 (over y, core).
Axes of the slice: x: 2, y: 2, z: 4, core: 2. Of those that a mesh axis runs over, the one named last changes fastest.
Arguments:
- amplitudes: float32 [2, 8388608], P(None, ('gx', 'gy', 'gz')), may hold values from -6 to 6
- couplings: float32 [23], replicated, may hold values from -1.2 to 1.2
- fields: float32 [23], replicated, may hold values from 0.3 to 1.2
Outputs:
- evolved: float32 [2, 8388608], P(None, ('gx', 'gy', 'gz'))
The draws below stay inside these ranges and needn't reach their ends.
All inputs are finite; a program needn't handle non-finite values.
Results may differ from the reference program's by a relative error of at most 0.000098.
Values sent between devices are 32-bit elements; how exact they have to be, the bound alone decides.
A program may use at most 64 MiB of HBM per device.

```python
import jax
import jax.numpy as jnp

NQ = 23
NAMP = 8388608


def levels(rng, shape, shards, least, high):
    factor_of, own = 1.0, jax.random.fold_in(rng, 6)
    for axis_at, parts in shards:
        heights = jnp.exp(jax.random.uniform(jax.random.fold_in(own, axis_at), (parts,), jnp.float32, least / len(shards), high / len(shards)))
        factor_of = factor_of * jnp.repeat(heights, shape[axis_at] // parts).reshape([-1 if axis == axis_at else 1 for axis in range(len(shape))])
    return factor_of


def normal_values(own_key, shape, width, most, shards=(), held_as=jnp.bfloat16):
    level = levels(own_key, shape, shards, -0.22, 0.18) if shards else 1.0
    entries = jax.random.normal(own_key, shape, jnp.float32) * width * level
    return jnp.minimum(jnp.maximum(entries, -most), most).astype(held_as)


def setup_inputs(seed: int = 0) -> dict:
    arg_keys = jax.random.split(jax.random.key(seed), 4)
    amplitudes = normal_values(arg_keys[0], (2, NAMP), 1.0, 6.0, ((1, 32),), jnp.float32)
    couplings = jnp.clip(jax.random.uniform(arg_keys[1], (NQ,), jnp.float32, -1.2, 1.2), -1.2, 1.2)
    fields = jnp.clip(jax.random.uniform(arg_keys[2], (NQ,), jnp.float32, 0.3, 1.2), 0.3, 1.2)
    return {"amplitudes": amplitudes, "couplings": couplings, "fields": fields}


def zz_phases(amplitudes, couplings):
    length_all = amplitudes.shape[1]
    qubits = couplings.shape[0]
    positions = jnp.arange(length_all, dtype=jnp.int32)
    phases = jnp.zeros((length_all,), jnp.float32)
    for bond_index in range(qubits):
        follow = (bond_index + 1) % qubits
        parity = ((positions >> bond_index) ^ (positions >> follow)) & 1
        phases = phases + couplings[bond_index] * (1.0 - 2.0 * parity.astype(jnp.float32))
    cos_phase = jnp.cos(phases)
    sin_phase = jnp.sin(phases)
    real_part = amplitudes[0] * cos_phase + amplitudes[1] * sin_phase
    imag_part = amplitudes[1] * cos_phase - amplitudes[0] * sin_phase
    return real_part, imag_part


def rotate_all(real_part, imag_part, fields):
    length_all = real_part.shape[0]
    for qubit_index in range(fields.shape[0]):
        cosine = jnp.cos(fields[qubit_index])
        sine_value = jnp.sin(fields[qubit_index])
        shape_now = (length_all >> (qubit_index + 1), 2, 1 << qubit_index)
        shaped_real = real_part.reshape(shape_now)
        shaped_imag = imag_part.reshape(shape_now)
        lower_real = shaped_real[:, 0]
        upper_real = shaped_real[:, 1]
        lower_imag = shaped_imag[:, 0]
        upper_imag = shaped_imag[:, 1]
        new_lower_real = cosine * lower_real + sine_value * upper_imag
        new_lower_imag = cosine * lower_imag - sine_value * upper_real
        new_upper_real = cosine * upper_real + sine_value * lower_imag
        new_upper_imag = cosine * upper_imag - sine_value * lower_real
        real_part = jnp.stack([new_lower_real, new_upper_real], axis=1).reshape(length_all)
        imag_part = jnp.stack([new_lower_imag, new_upper_imag], axis=1).reshape(length_all)
    return real_part, imag_part


def reference(amplitudes, couplings, fields):
    real_part, imag_part = zz_phases(amplitudes, couplings)
    real_part, imag_part = rotate_all(real_part, imag_part, fields)
    return jnp.stack([real_part, imag_part])
```

```python
import functools
import math

import jax
import jax.numpy as jnp
from jax import lax
from jax.experimental import pallas as pl
from jax.experimental.pallas import tpu as pltpu
from jax.sharding import PartitionSpec as P

MESH = pl.DeviceIdType.MESH
AXES = ("gx", "gy", "gz")
LANES = 128
CHUNK_BITS = 3
LOW_BITS = 5
EXACT = lax.Precision.HIGHEST


def log2(size):
    return size.bit_length() - 1


def bits_set(value, first, last):
    total = jnp.zeros_like(value)
    for bit in range(first, last):
        total = total + ((value >> bit) & 1)
    return total


def swapped(value):
    rows = value.shape[0]
    even = lax.broadcasted_iota(jnp.int32, value.shape, 0) & 1 == 0
    return jnp.where(even, pltpu.roll(value, rows - 1, 0), pltpu.roll(value, 1, 0))


def kernel(sizes, qubits, couplings, fields, amp, out, held, state, landed, done, low_c, low_s, high_c, high_s, cosine, sine, rows_w, lanes_w, in_sem, out_sem, send_sem, recv_sem):
    rows_all = held.shape[0]
    chunks = 1 << CHUNK_BITS
    chunk = rows_all // chunks
    lane_bits = log2(LANES)
    local_bits = log2(rows_all // 2) + lane_bits
    chunk_low = local_bits - CHUNK_BITS
    low_top = lane_bits + LOW_BITS
    tile = 2 << LOW_BITS
    highs = rows_all // tile
    place = {axis: lax.axis_index(axis) for axis in AXES}
    device = jnp.int32(0)
    for axis in AXES:
        device = device * sizes[axis] + place[axis]

    stages = {axis: [] for axis in AXES}
    qubit = local_bits
    for axis in reversed(AXES):
        for bit in range(log2(sizes[axis])):
            stages[axis].append((axis, bit, qubit))
            qubit += 1
    far = list(reversed(stages["gx"]))
    near = stages["gy"] + list(reversed(stages["gz"]))
    turn = near[1::-1] + near[2:]
    half = (len(far) + 1) // 2
    plans = (far[:half] + near + far[half:], far[half:] + turn + far[:half])
    count = len(plans[0])

    def partner(axis, bit):
        return tuple(place[a] ^ (1 << bit) if a == axis else place[a] for a in AXES)

    loads = [pltpu.make_async_copy(amp.at[pl.ds(c * chunk, chunk)], held.at[pl.ds(c * chunk, chunk)], in_sem.at[c]) for c in range(chunks)]
    for load in loads:
        load.start()
    barrier = pltpu.get_barrier_semaphore()
    for axis, bit, _ in plans[0]:
        pl.semaphore_signal(barrier, inc=1, device_id=partner(axis, bit), device_id_type=MESH)

    for q in range(qubits):
        cosine[pl.ds(q, 1), :] = jnp.full((1, LANES), fields[q], jnp.float32)
    angles = cosine[...]
    cosine[...] = jnp.cos(angles)
    sine[...] = jnp.sin(angles)

    def angle_of(position, bonds):
        total = jnp.zeros(position.shape, jnp.float32)
        for q in bonds:
            parity = (position >> q ^ position >> ((q + 1) % qubits)) & 1
            total = total + couplings[q] * (1.0 - 2.0 * parity.astype(jnp.float32))
        return total

    row = lax.broadcasted_iota(jnp.int32, (2 * tile, LANES), 0)
    lane = lax.broadcasted_iota(jnp.int32, (2 * tile, LANES), 1)
    position = (device << local_bits) + ((row >> 1) << lane_bits) + lane
    turns = bits_set(position, 0, low_top) & 3
    low = angle_of(position, list(range(low_top)) + [qubits - 1]) + turns.astype(jnp.float32) * (math.pi / 2)
    low_c[...] = jnp.cos(low)
    low_s[...] = jnp.sin(low)
    high_row = lax.broadcasted_iota(jnp.int32, (highs, LANES), 0)
    position = (device << local_bits) + (high_row << low_top)
    turns = bits_set(position, low_top, qubits) & 3
    high = angle_of(position, range(low_top, qubits - 1)) + turns.astype(jnp.float32) * (math.pi / 2)
    high_c[...] = jnp.cos(high)
    high_s[...] = jnp.sin(high)

    for load in loads:
        load.wait()

    @pl.loop(0, chunk // 8)
    def _(step):
        sign = jnp.where(lax.broadcasted_iota(jnp.int32, (8, LANES), 0) & 1 == 0, 1.0, -1.0)
        at = pl.multiple_of(step * 8, 8)
        low_at = pl.multiple_of(lax.rem(step * 8, 2 * tile), 8)
        c_low = low_c[pl.ds(low_at, 8), :]
        s_low = low_s[pl.ds(low_at, 8), :]
        high_at = step * 8 // tile
        parts = []
        for c in range(chunks):
            number = c * (chunk // tile) + high_at
            c_high = high_c[pl.ds(number, 1), :]
            s_high = high_s[pl.ds(number, 1), :]
            value = held[pl.ds(pl.multiple_of(c * chunk + at, 8), 8), :]
            c_all = c_low * c_high - s_low * s_high
            s_all = s_low * c_high + c_low * s_high
            parts.append(value * c_all + swapped(value) * (s_all * sign))
        for bit in range(CHUNK_BITS):
            c_q = cosine[pl.ds(chunk_low + bit, 1), :]
            s_q = sine[pl.ds(chunk_low + bit, 1), :]
            mixed = list(parts)
            for c in range(chunks):
                if not c >> bit & 1:
                    first, second = parts[c], parts[c | 1 << bit]
                    mixed[c] = c_q * first + s_q * second
                    mixed[c | 1 << bit] = s_q * first - c_q * second
            parts = mixed
        for c in range(chunks):
            state[0, pl.ds(pl.multiple_of(c * chunk + at, 8), 8), :] = parts[c]

    def send(c, k):
        axis, bit, _ = plans[c % 2][k]
        span = pl.ds(c * chunk, chunk)
        return pltpu.make_async_remote_copy(
            src_ref=state.at[k, span],
            dst_ref=landed.at[k, span],
            send_sem=send_sem.at[k, c],
            recv_sem=recv_sem.at[k, c],
            device_id=partner(axis, bit),
            device_id_type=MESH,
        )

    pl.semaphore_wait(barrier, count)
    for c in range(chunks):
        send(c, 0).start()

    def matrix(shape, first_row, skip, first, last):
        there = lax.broadcasted_iota(jnp.int32, shape, 0) + first_row
        here = lax.broadcasted_iota(jnp.int32, shape, 1)
        total = jnp.ones(shape, jnp.float32)
        if skip:
            total = jnp.where((there ^ here) & ((1 << skip) - 1) == 0, total, 0.0)
        repeat = shape[1] // LANES
        for q in range(first, last):
            bit = q - first + skip
            c_q = jnp.concatenate([cosine[pl.ds(q, 1), :]] * repeat, axis=1)
            s_q = jnp.concatenate([sine[pl.ds(q, 1), :]] * repeat, axis=1)
            up, left = there >> bit & 1, here >> bit & 1
            total = total * jnp.where(up ^ left == 1, s_q, jnp.where(up == 1, -c_q, c_q))
        return total

    lanes_w[...] = matrix((LANES, LANES), 0, 0, 0, lane_bits)

    @pl.loop(0, chunk // 8)
    def _(step):
        at = pl.multiple_of(step * 8, 8)
        rows_w[pl.ds(at, 8), :] = matrix((8, chunk), at, 1, lane_bits, chunk_low)

    block = LANES

    def local(c, source, target):
        @pl.loop(0, chunk // block)
        def _(step):
            at = pl.multiple_of(c * chunk + step * block, block)
            source[pl.ds(at, block), :] = jnp.dot(source[pl.ds(at, block), :], lanes_w[...], precision=EXACT, preferred_element_type=jnp.float32)

        @pl.loop(0, chunk // block)
        def _(step):
            at = pl.multiple_of(step * block, block)
            target[pl.ds(pl.multiple_of(c * chunk + at, block), block), :] = jnp.dot(
                rows_w[pl.ds(at, block), :], source[pl.ds(c * chunk, chunk), :], precision=EXACT, preferred_element_type=jnp.float32
            )

    def combine(c, k, target, last):
        axis, bit, q = plans[c % 2][k]
        own = 1.0 - 2.0 * ((place[axis] >> bit) & 1).astype(jnp.float32)

        @pl.loop(0, chunk // tile)
        def _(step):
            at = pl.multiple_of(c * chunk + step * tile, tile)
            c_q = cosine[pl.ds(q, 1), :] * own
            s_q = sine[pl.ds(q, 1), :]
            value = c_q * state[k, pl.ds(at, tile), :] + s_q * landed[k, pl.ds(at, tile), :]
            if last:
                row = lax.broadcasted_iota(jnp.int32, (tile, LANES), 0)
                lane = lax.broadcasted_iota(jnp.int32, (tile, LANES), 1)
                inner = ((row >> 1) << lane_bits) + lane
                number = (device << local_bits) + ((c * (chunk // tile) + step) << low_top)
                turns = bits_set(inner, 0, low_top) + bits_set(number, low_top, qubits)
                value = jnp.where(turns & 1 == 1, swapped(value), value)
                value = jnp.where((turns + (row & 1)) & 2 == 2, -value, value)
            target[pl.ds(at, tile), :] = value

    events = [(c // 2 + 0.5 * k if k < count - 1 else 2 * chunks + c // 2, k, c) for c in range(chunks) for k in range(count)]
    stores = []
    for _, k, c in sorted(events):
        send(c, k).wait_recv()
        if k == count - 1:
            combine(c, k, done, True)
            span = pl.ds(c * chunk, chunk)
            stores.append(pltpu.make_async_copy(done.at[span], out.at[span], out_sem.at[c]))
            stores[-1].start()
        elif k == 0:
            combine(c, k, done, False)
            local(c, done, state.at[1])
            send(c, 1).start()
        else:
            combine(c, k, state.at[k + 1], False)
            send(c, k + 1).start()
    for k in range(count):
        for c in range(chunks):
            send(c, k).wait_send()
    for store in stores:
        store.wait()


def solution(mesh):
    sizes = {axis: mesh.shape[axis] for axis in AXES}
    count = sum(log2(size) for size in sizes.values())

    def step(amplitudes, couplings, fields):
        local = amplitudes.shape[1]
        qubits = couplings.shape[0]
        rows = 2 * local // LANES
        chunks = 1 << CHUNK_BITS
        chunk = rows // chunks
        tile = 2 << LOW_BITS
        table = -(-qubits // 8) * 8
        woven = amplitudes.reshape(2, local // LANES, LANES).transpose(1, 0, 2).reshape(rows, LANES)
        vmem = lambda *shape: pltpu.VMEM(shape, jnp.float32)
        result = pl.pallas_call(
            functools.partial(kernel, sizes, qubits),
            out_shape=jax.ShapeDtypeStruct((rows, LANES), jnp.float32),
            in_specs=[pl.BlockSpec(memory_space=pltpu.SMEM)] * 2 + [pl.BlockSpec(memory_space=pl.ANY)],
            out_specs=pl.BlockSpec(memory_space=pl.ANY),
            scratch_shapes=[
                vmem(rows, LANES),
                vmem(count, rows, LANES),
                vmem(count, rows, LANES),
                vmem(rows, LANES),
                vmem(2 * tile, LANES),
                vmem(2 * tile, LANES),
                vmem(rows // tile, LANES),
                vmem(rows // tile, LANES),
                vmem(table, LANES),
                vmem(table, LANES),
                vmem(chunk, chunk),
                vmem(LANES, LANES),
                pltpu.SemaphoreType.DMA((chunks,)),
                pltpu.SemaphoreType.DMA((chunks,)),
                pltpu.SemaphoreType.DMA((count, chunks)),
                pltpu.SemaphoreType.DMA((count, chunks)),
            ],
            compiler_params=pltpu.CompilerParams(
                collective_id=0, has_side_effects=True, vmem_limit_bytes=60 << 20
            ),
        )(couplings, fields, woven)
        return result.reshape(local // LANES, 2, LANES).transpose(1, 0, 2).reshape(2, local)

    placed = (P(None, AXES), P(), P())
    return jax.shard_map(step, mesh=mesh, in_specs=placed, out_specs=P(None, AXES), check_vma=False)
```

```python
import functools
import math

import jax
import jax.numpy as jnp
from jax import lax
from jax.experimental import pallas as pl
from jax.experimental.pallas import tpu as pltpu
from jax.sharding import PartitionSpec as P

MESH = pl.DeviceIdType.MESH
AXES = ("gx", "gy", "gz")
LANES = 128
CHUNK_BITS = 3
LOW_BITS = 5
VMEM = 67043328
EXACT = lax.Precision.HIGHEST


def log2(size):
    return size.bit_length() - 1


def bits_set(value, first, last):
    total = jnp.zeros_like(value)
    for bit in range(first, last):
        total = total + ((value >> bit) & 1)
    return total


def swapped(value):
    rows = value.shape[0]
    even = lax.broadcasted_iota(jnp.int32, value.shape, 0) & 1 == 0
    return jnp.where(even, pltpu.roll(value, rows - 1, 0), pltpu.roll(value, 1, 0))


def kernel(sizes, qubits, couplings, fields, amp, done, held, state, landed, low_c, low_s, high_c, high_s, cosine, sine, rows_w, lanes_w, in_sem, send_sem, recv_sem):
    rows_all = held.shape[0]
    chunks = 1 << CHUNK_BITS
    chunk = rows_all // chunks
    lane_bits = log2(LANES)
    local_bits = log2(rows_all // 2) + lane_bits
    chunk_low = local_bits - CHUNK_BITS
    low_top = lane_bits + LOW_BITS
    tile = 2 << LOW_BITS
    highs = rows_all // tile
    place = {axis: lax.axis_index(axis) for axis in AXES}
    device = jnp.int32(0)
    for axis in AXES:
        device = device * sizes[axis] + place[axis]

    stages = {axis: [] for axis in AXES}
    qubit = local_bits
    for axis in reversed(AXES):
        for bit in range(log2(sizes[axis])):
            stages[axis].append((axis, bit, qubit))
            qubit += 1
    far = list(reversed(stages["gx"]))
    near = stages["gy"] + list(reversed(stages["gz"]))
    turn = near[1::-1] + near[2:]
    half = (len(far) + 1) // 2
    plans = (far[:half] + near + far[half:], far[half:] + turn + far[:half])
    count = len(plans[0])

    def partner(axis, bit):
        return tuple(place[a] ^ (1 << bit) if a == axis else place[a] for a in AXES)

    loads = [pltpu.make_async_copy(amp.at[pl.ds(c * chunk, chunk)], held.at[pl.ds(c * chunk, chunk)], in_sem.at[c]) for c in range(chunks)]
    for load in loads:
        load.start()
    barrier = pltpu.get_barrier_semaphore()
    for axis, bit, _ in plans[0]:
        pl.semaphore_signal(barrier, inc=1, device_id=partner(axis, bit), device_id_type=MESH)

    for q in range(qubits):
        cosine[pl.ds(q, 1), :] = jnp.full((1, LANES), fields[q], jnp.float32)
    angles = cosine[...]
    cosine[...] = jnp.cos(angles)
    sine[...] = jnp.sin(angles)

    def angle_of(position, bonds):
        total = jnp.zeros(position.shape, jnp.float32)
        for q in bonds:
            parity = (position >> q ^ position >> ((q + 1) % qubits)) & 1
            total = total + couplings[q] * (1.0 - 2.0 * parity.astype(jnp.float32))
        return total

    row = lax.broadcasted_iota(jnp.int32, (2 * tile, LANES), 0)
    lane = lax.broadcasted_iota(jnp.int32, (2 * tile, LANES), 1)
    position = (device << local_bits) + ((row >> 1) << lane_bits) + lane
    turns = bits_set(position, 0, low_top) & 3
    low = angle_of(position, list(range(low_top)) + [qubits - 1]) + turns.astype(jnp.float32) * (math.pi / 2)
    low_c[...] = jnp.cos(low)
    low_s[...] = jnp.sin(low)
    high_row = lax.broadcasted_iota(jnp.int32, (highs, LANES), 0)
    position = (device << local_bits) + (high_row << low_top)
    turns = bits_set(position, low_top, qubits) & 3
    high = angle_of(position, range(low_top, qubits - 1)) + turns.astype(jnp.float32) * (math.pi / 2)
    high_c[...] = jnp.cos(high)
    high_s[...] = jnp.sin(high)

    for load in loads:
        load.wait()

    @pl.loop(0, chunk // 8)
    def _(step):
        sign = jnp.where(lax.broadcasted_iota(jnp.int32, (8, LANES), 0) & 1 == 0, 1.0, -1.0)
        at = pl.multiple_of(step * 8, 8)
        low_at = pl.multiple_of(lax.rem(step * 8, 2 * tile), 8)
        c_low = low_c[pl.ds(low_at, 8), :]
        s_low = low_s[pl.ds(low_at, 8), :]
        high_at = step * 8 // tile
        parts = []
        for c in range(chunks):
            number = c * (chunk // tile) + high_at
            c_high = high_c[pl.ds(number, 1), :]
            s_high = high_s[pl.ds(number, 1), :]
            value = held[pl.ds(pl.multiple_of(c * chunk + at, 8), 8), :]
            c_all = c_low * c_high - s_low * s_high
            s_all = s_low * c_high + c_low * s_high
            parts.append(value * c_all + swapped(value) * (s_all * sign))
        for bit in range(CHUNK_BITS):
            c_q = cosine[pl.ds(chunk_low + bit, 1), :]
            s_q = sine[pl.ds(chunk_low + bit, 1), :]
            mixed = list(parts)
            for c in range(chunks):
                if not c >> bit & 1:
                    first, second = parts[c], parts[c | 1 << bit]
                    mixed[c] = c_q * first + s_q * second
                    mixed[c | 1 << bit] = s_q * first - c_q * second
            parts = mixed
        for c in range(chunks):
            state[0, pl.ds(pl.multiple_of(c * chunk + at, 8), 8), :] = parts[c]

    def send(c, k):
        axis, bit, _ = plans[c % 2][k]
        span = pl.ds(c * chunk, chunk)
        return pltpu.make_async_remote_copy(
            src_ref=state.at[k, span],
            dst_ref=landed.at[k, span],
            send_sem=send_sem.at[k, c],
            recv_sem=recv_sem.at[k, c],
            device_id=partner(axis, bit),
            device_id_type=MESH,
        )

    pl.semaphore_wait(barrier, count)
    for c in range(chunks):
        send(c, 0).start()

    def matrix(shape, first_row, skip, first, last):
        there = lax.broadcasted_iota(jnp.int32, shape, 0) + first_row
        here = lax.broadcasted_iota(jnp.int32, shape, 1)
        total = jnp.ones(shape, jnp.float32)
        if skip:
            total = jnp.where((there ^ here) & ((1 << skip) - 1) == 0, total, 0.0)
        repeat = shape[1] // LANES
        for q in range(first, last):
            bit = q - first + skip
            c_q = jnp.concatenate([cosine[pl.ds(q, 1), :]] * repeat, axis=1)
            s_q = jnp.concatenate([sine[pl.ds(q, 1), :]] * repeat, axis=1)
            up, left = there >> bit & 1, here >> bit & 1
            total = total * jnp.where(up ^ left == 1, s_q, jnp.where(up == 1, -c_q, c_q))
        return total

    lanes_w[...] = matrix((LANES, LANES), 0, 0, 0, lane_bits)

    @pl.loop(0, chunk // 8)
    def _(step):
        at = pl.multiple_of(step * 8, 8)
        rows_w[pl.ds(at, 8), :] = matrix((8, chunk), at, 1, lane_bits, chunk_low)

    block = LANES

    def local(c, source, target):
        @pl.loop(0, chunk // block)
        def _(step):
            at = pl.multiple_of(c * chunk + step * block, block)
            source[pl.ds(at, block), :] = jnp.dot(source[pl.ds(at, block), :], lanes_w[...], precision=EXACT, preferred_element_type=jnp.float32)

        @pl.loop(0, chunk // block)
        def _(step):
            at = pl.multiple_of(step * block, block)
            target[pl.ds(pl.multiple_of(c * chunk + at, block), block), :] = jnp.dot(
                rows_w[pl.ds(at, block), :], source[pl.ds(c * chunk, chunk), :], precision=EXACT, preferred_element_type=jnp.float32
            )

    def combine(c, k, target, last):
        axis, bit, q = plans[c % 2][k]
        own = 1.0 - 2.0 * ((place[axis] >> bit) & 1).astype(jnp.float32)

        @pl.loop(0, chunk // tile)
        def _(step):
            at = pl.multiple_of(c * chunk + step * tile, tile)
            c_q = cosine[pl.ds(q, 1), :] * own
            s_q = sine[pl.ds(q, 1), :]
            value = c_q * state[k, pl.ds(at, tile), :] + s_q * landed[k, pl.ds(at, tile), :]
            if last:
                row = lax.broadcasted_iota(jnp.int32, (tile, LANES), 0)
                lane = lax.broadcasted_iota(jnp.int32, (tile, LANES), 1)
                inner = ((row >> 1) << lane_bits) + lane
                number = (device << local_bits) + ((c * (chunk // tile) + step) << low_top)
                turns = bits_set(inner, 0, low_top) + bits_set(number, low_top, qubits)
                value = jnp.where(turns & 1 == 1, swapped(value), value)
                value = jnp.where((turns + (row & 1)) & 2 == 2, -value, value)
            target[pl.ds(at, tile), :] = value

    events = [(c // 2 + 0.5 * k if k < count - 1 else 2 * chunks + c // 2, k, c) for c in range(chunks) for k in range(count)]
    for _, k, c in sorted(events):
        send(c, k).wait_recv()
        if k == count - 1:
            combine(c, k, done, True)
        elif k == 0:
            combine(c, k, done, False)
            local(c, done, state.at[1])
            send(c, 1).start()
        else:
            combine(c, k, state.at[k + 1], False)
            send(c, k + 1).start()
    for k in range(count):
        for c in range(chunks):
            send(c, k).wait_send()


def solution(mesh):
    sizes = {axis: mesh.shape[axis] for axis in AXES}
    count = sum(log2(size) for size in sizes.values())

    def step(amplitudes, couplings, fields):
        local = amplitudes.shape[1]
        qubits = couplings.shape[0]
        rows = 2 * local // LANES
        chunks = 1 << CHUNK_BITS
        chunk = rows // chunks
        tile = 2 << LOW_BITS
        table = -(-qubits // 8) * 8
        woven = amplitudes.reshape(2, local // LANES, LANES).transpose(1, 0, 2).reshape(rows, LANES)
        vmem = lambda *shape: pltpu.VMEM(shape, jnp.float32)
        result = pl.pallas_call(
            functools.partial(kernel, sizes, qubits),
            out_shape=pltpu.VMEM((rows, LANES), jnp.float32),
            in_specs=[pl.BlockSpec(memory_space=pltpu.SMEM)] * 2 + [pl.BlockSpec(memory_space=pltpu.HBM)],
            out_specs=pl.BlockSpec(memory_space=pltpu.VMEM),
            scratch_shapes=[
                vmem(rows, LANES),
                vmem(count, rows, LANES),
                vmem(count, rows, LANES),
                vmem(2 * tile, LANES),
                vmem(2 * tile, LANES),
                vmem(rows // tile, LANES),
                vmem(rows // tile, LANES),
                vmem(table, LANES),
                vmem(table, LANES),
                vmem(chunk, chunk),
                vmem(LANES, LANES),
                pltpu.SemaphoreType.DMA((chunks,)),
                pltpu.SemaphoreType.DMA((count, chunks)),
                pltpu.SemaphoreType.DMA((count, chunks)),
            ],
            compiler_params=pltpu.CompilerParams(
                collective_id=0, has_side_effects=True, vmem_limit_bytes=VMEM - 4 * rows * LANES
            ),
        )(couplings, fields, woven)
        return result.reshape(local // LANES, 2, LANES).transpose(1, 0, 2).reshape(2, local)

    placed = (P(None, AXES), P(), P())
    return jax.shard_map(step, mesh=mesh, in_specs=placed, out_specs=P(None, AXES), check_vma=False)
```

```python
import functools
import math

import jax
import jax.numpy as jnp
from jax import lax
from jax.experimental import pallas as pl
from jax.experimental.pallas import tpu as pltpu
from jax.sharding import PartitionSpec as P

MESH = pl.DeviceIdType.MESH
AXES = ("gx", "gy", "gz")
LANES = 128
CHUNK_BITS = 3
LOW_BITS = 5
VMEM = 67043328
EXACT = lax.Precision.HIGHEST


def log2(size):
    return size.bit_length() - 1


def bits_set(value, first, last):
    total = jnp.zeros_like(value)
    for bit in range(first, last):
        total = total + ((value >> bit) & 1)
    return total


def swapped(value):
    rows = value.shape[0]
    even = lax.broadcasted_iota(jnp.int32, value.shape, 0) & 1 == 0
    return jnp.where(even, pltpu.roll(value, rows - 1, 0), pltpu.roll(value, 1, 0))


def kernel(sizes, qubits, couplings, fields, amp, done, held, state, landed, low_c, low_s, high_c, high_s, cosine, sine, rows_w, lanes_w, in_sem, send_sem, recv_sem, far_send, far_recv):
    rows_all = held.shape[0]
    chunks = 1 << CHUNK_BITS
    chunk = rows_all // chunks
    lane_bits = log2(LANES)
    local_bits = log2(rows_all // 2) + lane_bits
    chunk_low = local_bits - CHUNK_BITS
    low_top = lane_bits + LOW_BITS
    tile = 2 << LOW_BITS
    highs = rows_all // tile
    place = {axis: lax.axis_index(axis) for axis in AXES}
    device = jnp.int32(0)
    for axis in AXES:
        device = device * sizes[axis] + place[axis]

    stages = {axis: [] for axis in AXES}
    qubit = local_bits
    for axis in reversed(AXES):
        for bit in range(log2(sizes[axis])):
            stages[axis].append((axis, bit, qubit))
            qubit += 1
    near = stages["gy"] + list(reversed(stages["gz"]))
    plans = (near, near[1::-1] + near[2:])
    count = len(near)
    parts_gx = sizes["gx"]
    far_bits = log2(parts_gx)
    part = chunk // parts_gx
    part_low = chunk_low - far_bits
    own = place["gx"]

    def partner(axis, bit):
        return tuple(place[a] ^ (1 << bit) if a == axis else place[a] for a in AXES)

    def distant(apart):
        return tuple(place[a] ^ apart if a == "gx" else place[a] for a in AXES)

    loads = [pltpu.make_async_copy(amp.at[pl.ds(c * chunk, chunk)], held.at[pl.ds(c * chunk, chunk)], in_sem.at[c]) for c in range(chunks)]
    for load in loads:
        load.start()
    barrier = pltpu.get_barrier_semaphore()
    for axis, bit, _ in near:
        pl.semaphore_signal(barrier, inc=1, device_id=partner(axis, bit), device_id_type=MESH)
    for apart in range(1, parts_gx):
        pl.semaphore_signal(barrier, inc=1, device_id=distant(apart), device_id_type=MESH)

    for q in range(qubits):
        cosine[pl.ds(q, 1), :] = jnp.full((1, LANES), fields[q], jnp.float32)
    angles = cosine[...]
    cosine[...] = jnp.cos(angles)
    sine[...] = jnp.sin(angles)

    def angle_of(position, bonds):
        total = jnp.zeros(position.shape, jnp.float32)
        for q in bonds:
            parity = (position >> q ^ position >> ((q + 1) % qubits)) & 1
            total = total + couplings[q] * (1.0 - 2.0 * parity.astype(jnp.float32))
        return total

    row = lax.broadcasted_iota(jnp.int32, (2 * tile, LANES), 0)
    lane = lax.broadcasted_iota(jnp.int32, (2 * tile, LANES), 1)
    position = (device << local_bits) + ((row >> 1) << lane_bits) + lane
    turns = bits_set(position, 0, low_top) & 3
    low = angle_of(position, list(range(low_top)) + [qubits - 1]) + turns.astype(jnp.float32) * (math.pi / 2)
    low_c[...] = jnp.cos(low)
    low_s[...] = jnp.sin(low)
    high_row = lax.broadcasted_iota(jnp.int32, (highs, LANES), 0)
    position = (device << local_bits) + (high_row << low_top)
    turns = bits_set(position, low_top, qubits) & 3
    high = angle_of(position, range(low_top, qubits - 1)) + turns.astype(jnp.float32) * (math.pi / 2)
    high_c[...] = jnp.cos(high)
    high_s[...] = jnp.sin(high)

    for load in loads:
        load.wait()

    def mix(parts, qubit):
        for bit in range(log2(len(parts))):
            c_q = cosine[pl.ds(qubit + bit, 1), :]
            s_q = sine[pl.ds(qubit + bit, 1), :]
            mixed = list(parts)
            for p in range(len(parts)):
                if not p >> bit & 1:
                    first, second = parts[p], parts[p | 1 << bit]
                    mixed[p] = c_q * first + s_q * second
                    mixed[p | 1 << bit] = s_q * first - c_q * second
            parts = mixed
        return parts

    @pl.loop(0, chunk // 8)
    def _(step):
        sign = jnp.where(lax.broadcasted_iota(jnp.int32, (8, LANES), 0) & 1 == 0, 1.0, -1.0)
        at = pl.multiple_of(step * 8, 8)
        low_at = pl.multiple_of(lax.rem(step * 8, 2 * tile), 8)
        c_low = low_c[pl.ds(low_at, 8), :]
        s_low = low_s[pl.ds(low_at, 8), :]
        high_at = step * 8 // tile
        parts = []
        for c in range(chunks):
            number = c * (chunk // tile) + high_at
            c_high = high_c[pl.ds(number, 1), :]
            s_high = high_s[pl.ds(number, 1), :]
            value = held[pl.ds(pl.multiple_of(c * chunk + at, 8), 8), :]
            c_all = c_low * c_high - s_low * s_high
            s_all = s_low * c_high + c_low * s_high
            parts.append(value * c_all + swapped(value) * (s_all * sign))
        parts = mix(parts, chunk_low)
        for c in range(chunks):
            state[0, pl.ds(pl.multiple_of(c * chunk + at, 8), 8), :] = parts[c]

    def send(c, k):
        axis, bit, _ = plans[c % 2][k - 1]
        span = pl.ds(c * chunk, chunk)
        return pltpu.make_async_remote_copy(
            src_ref=state.at[k, span],
            dst_ref=landed.at[k, span],
            send_sem=send_sem.at[k, c],
            recv_sem=recv_sem.at[k, c],
            device_id=partner(axis, bit),
            device_id_type=MESH,
        )

    def cross(c, apart, back):
        theirs = pl.ds(pl.multiple_of(c * chunk + (own ^ apart) * part, 8), part)
        mine = pl.ds(pl.multiple_of(c * chunk + own * part, 8), part)
        return pltpu.make_async_remote_copy(
            src_ref=state.at[count + 1 if back else 0, theirs],
            dst_ref=done.at[mine] if back else landed.at[0, mine],
            send_sem=far_send.at[back, apart, c],
            recv_sem=far_recv.at[back, apart, c],
            device_id=distant(apart),
            device_id_type=MESH,
        )

    def premix(c):
        @pl.loop(0, part // 8)
        def _(step):
            spans = [pl.ds(pl.multiple_of(c * chunk + p * part + step * 8, 8), 8) for p in range(parts_gx)]
            for span, value in zip(spans, mix([state[0, span, :] for span in spans], part_low)):
                state[0, span, :] = value

    premix(0)
    pl.semaphore_wait(barrier, count + parts_gx - 1)
    for c in range(chunks):
        if c:
            premix(c)
        for apart in reversed(range(1, parts_gx)):
            cross(c, apart, 0).start()

    def matrix(shape, first_row, skip, kept):
        there = lax.broadcasted_iota(jnp.int32, shape, 0) + first_row
        here = lax.broadcasted_iota(jnp.int32, shape, 1)
        total = jnp.ones(shape, jnp.float32)
        if skip:
            total = jnp.where((there ^ here) & ((1 << skip) - 1) == 0, total, 0.0)
        repeat = shape[1] // LANES
        for bit, q in enumerate(kept, skip):
            c_q = jnp.concatenate([cosine[pl.ds(q, 1), :]] * repeat, axis=1)
            s_q = jnp.concatenate([sine[pl.ds(q, 1), :]] * repeat, axis=1)
            up, left = there >> bit & 1, here >> bit & 1
            total = total * jnp.where(up ^ left == 1, s_q, jnp.where(up == 1, -c_q, c_q))
        return total

    lanes_w[...] = matrix((LANES, LANES), 0, 0, range(lane_bits))

    inside = list(range(lane_bits, part_low)) + list(range(qubits - far_bits, qubits))

    @pl.loop(0, chunk // 8)
    def _(step):
        at = pl.multiple_of(step * 8, 8)
        rows_w[pl.ds(at, 8), :] = matrix((8, chunk), at, 1, inside)

    block = LANES

    def local(c, source, target):
        @pl.loop(0, chunk // block)
        def _(step):
            at = pl.multiple_of(c * chunk + step * block, block)
            source[pl.ds(at, block), :] = jnp.dot(source[pl.ds(at, block), :], lanes_w[...], precision=EXACT, preferred_element_type=jnp.float32)

        @pl.loop(0, chunk // block)
        def _(step):
            at = pl.multiple_of(step * block, block)
            target[pl.ds(pl.multiple_of(c * chunk + at, block), block), :] = jnp.dot(
                rows_w[pl.ds(at, block), :], source[pl.ds(c * chunk, chunk), :], precision=EXACT, preferred_element_type=jnp.float32
            )

    def combine(c, k, last):
        axis, bit, q = plans[c % 2][k - 1]
        side = 1.0 - 2.0 * ((place[axis] >> bit) & 1).astype(jnp.float32)

        @pl.loop(0, chunk // tile)
        def _(step):
            at = pl.multiple_of(c * chunk + step * tile, tile)
            c_q = cosine[pl.ds(q, 1), :] * side
            s_q = sine[pl.ds(q, 1), :]
            value = c_q * state[k, pl.ds(at, tile), :] + s_q * landed[k, pl.ds(at, tile), :]
            if last:
                row = lax.broadcasted_iota(jnp.int32, (tile, LANES), 0) + step * tile
                lane = lax.broadcasted_iota(jnp.int32, (tile, LANES), 1)
                owner = row // part
                home = c * chunk + own * part + row - owner * part
                turns = bits_set((home >> 1 << lane_bits) + lane, 0, local_bits)
                turns = turns + bits_set(owner, 0, far_bits) + bits_set(device & (1 << count) - 1, 0, count)
                value = jnp.where(turns & 1 == 1, swapped(value), value)
                value = jnp.where((turns + (row & 1)) & 2 == 2, -value, value)
            state[k + 1, pl.ds(at, tile), :] = value

    for _, k, c in sorted((c + k, k, c) for c in range(chunks) for k in range(count + 1)):
        mine = pl.ds(pl.multiple_of(c * chunk + own * part, 8), part)
        if k == 0:
            landed[0, mine, :] = state[0, mine, :]
            for apart in range(1, parts_gx):
                cross(c, apart, 0).wait_recv()
            local(c, landed.at[0], state.at[1])
        else:
            send(c, k).wait_recv()
            combine(c, k, k == count)
        if k < count:
            send(c, k + 1).start()
        else:
            for apart in reversed(range(1, parts_gx)):
                cross(c, apart, 1).start()
            done[mine, :] = state[count + 1, mine, :]
    for c in range(chunks):
        for k in range(1, count + 1):
            send(c, k).wait_send()
        for apart in range(1, parts_gx):
            cross(c, apart, 0).wait_send()
            cross(c, apart, 1).wait_send()
    for c in range(chunks):
        for apart in range(1, parts_gx):
            cross(c, apart, 1).wait_recv()


def solution(mesh):
    sizes = {axis: mesh.shape[axis] for axis in AXES}
    count = log2(sizes["gy"]) + log2(sizes["gz"])

    def step(amplitudes, couplings, fields):
        local = amplitudes.shape[1]
        qubits = couplings.shape[0]
        rows = 2 * local // LANES
        chunks = 1 << CHUNK_BITS
        chunk = rows // chunks
        tile = 2 << LOW_BITS
        table = -(-qubits // 8) * 8
        woven = amplitudes.reshape(2, local // LANES, LANES).transpose(1, 0, 2).reshape(rows, LANES)
        vmem = lambda *shape: pltpu.VMEM(shape, jnp.float32)
        result = pl.pallas_call(
            functools.partial(kernel, sizes, qubits),
            out_shape=pltpu.VMEM((rows, LANES), jnp.float32),
            in_specs=[pl.BlockSpec(memory_space=pltpu.SMEM)] * 2 + [pl.BlockSpec(memory_space=pltpu.HBM)],
            out_specs=pl.BlockSpec(memory_space=pltpu.VMEM),
            scratch_shapes=[
                vmem(rows, LANES),
                vmem(count + 2, rows, LANES),
                vmem(count + 1, rows, LANES),
                vmem(2 * tile, LANES),
                vmem(2 * tile, LANES),
                vmem(rows // tile, LANES),
                vmem(rows // tile, LANES),
                vmem(table, LANES),
                vmem(table, LANES),
                vmem(chunk, chunk),
                vmem(LANES, LANES),
                pltpu.SemaphoreType.DMA((chunks,)),
                pltpu.SemaphoreType.DMA((count + 1, chunks)),
                pltpu.SemaphoreType.DMA((count + 1, chunks)),
                pltpu.SemaphoreType.DMA((2, sizes["gx"], chunks)),
                pltpu.SemaphoreType.DMA((2, sizes["gx"], chunks)),
            ],
            compiler_params=pltpu.CompilerParams(
                collective_id=0, has_side_effects=True, vmem_limit_bytes=VMEM - 4 * rows * LANES
            ),
        )(couplings, fields, woven)
        return result.reshape(local // LANES, 2, LANES).transpose(1, 0, 2).reshape(2, local)

    placed = (P(None, AXES), P(), P())
    return jax.shard_map(step, mesh=mesh, in_specs=placed, out_specs=P(None, AXES), check_vma=False)
```
